128 devices in a mesh: dp: 4 (over x), cp: 32 (over z, y, core).
Axes of the slice: x: 4, y: 4, z: 4, core: 2. Of those that a mesh axis runs over, the one named last changes fastest.
Arguments:
- tokens: bfloat16 [4, 4096, 4096], P('dp', 'cp'), may hold values from -60 to 60
- qkv_weight: bfloat16 [4096, 3072], replicated, may hold values from -0.09375 to 0.09375
- owner_slot: int32 [4, 32], P('dp', 'cp'), may hold values from 0 to 3, as said below
- slab_sequence: int32 [4, 32], replicated, may hold values from 0 to 16, as said below
- slab_order: int32 [4, 32], replicated, may hold values from 0 to 15, as said below
Outputs:
- context: bfloat16 [4, 4096, 2048], P('dp', 'cp')
The draws below stay inside these ranges and needn't reach their ends.
Inputs may be any that keep to these rules, and one draw needn't show every extreme that they name: For every column c, the entries owner_slot[a, c] over all rows a are 0 to 3, each once. `slab_sequence`: in each row, the slabs with one sequence number carry the orders 0 to L-1, each once, L being their count; no sequence has more than 16 slabs. `slab_order`: see slab_sequence.
All inputs are finite; a program needn't handle non-finite values.
Results may differ from the reference program's by a relative error of at most 0.006.
The reference program's roundings to bfloat16 on the way count: a program that leaves them out, or rounds other values in their place, can miss the bound.
Values may be sent and summed in bfloat16 or wider, within the bound.
A program may use at most 128 MiB of HBM per device.

```python
import jax
import jax.numpy as jnp
from jax import lax

D = 4096
QH = 16
KVH = 4
HD = 128
SLAB = 128
SLABS_DEV = 1
GROUPS = 4
ROW_SLABS = 32
ROW_TOK = 4096


def sequence_plan(key):
    half_count = ROW_SLABS // 2
    chosen_row = jax.random.randint(jax.random.fold_in(key, 9), (), 0, GROUPS)
    singles_flags = jnp.arange(GROUPS, dtype=jnp.int32) == chosen_row

    def one_row(row_key, singles):
        first_key, second_key = jax.random.split(row_key)
        index = jnp.arange(ROW_SLABS, dtype=jnp.int32)
        random_starts = jax.random.randint(first_key, (ROW_SLABS,), 0, 8) == 0
        later_starts = random_starts | (index == half_count) | singles
        starts = jnp.where(index < half_count, index == 0, later_starts)
        numbers = jnp.cumsum(starts.astype(jnp.int32)) - 1
        begins = lax.cummax(jnp.where(starts, index, 0))
        shuffle = jax.random.permutation(second_key, ROW_SLABS)
        return (numbers[shuffle].astype(jnp.int32), (index - begins)[shuffle].astype(jnp.int32))
    return jax.vmap(one_row)(jax.random.split(jax.random.fold_in(key, 7), GROUPS), singles_flags)


def draw_slab_sequence(key, part):
    return sequence_plan(key)[0]


def draw_slab_order(key, part):
    return sequence_plan(key)[1]


def draw_owner_slot(key, part):
    columns_count = ROW_SLABS // SLABS_DEV
    column_keys = jax.random.split(jax.random.fold_in(key, 3), columns_count)

    def one_column(column_key):
        return jax.random.permutation(column_key, GROUPS * SLABS_DEV).astype(jnp.int32).reshape(GROUPS, SLABS_DEV)
    stacked = jax.vmap(one_column)(column_keys)
    return stacked.transpose(1, 0, 2).reshape(GROUPS, ROW_SLABS)


def draw_tokens(key, part):
    first_key, second_key = jax.random.split(jax.random.fold_in(key, 11))
    values = jax.random.normal(first_key, (GROUPS, ROW_TOK, D), jnp.float32)
    values = jnp.clip(values, -6.0, 6.0)
    return values.astype(jnp.bfloat16)


def scatter_about(stream_key, extent, spread, most, kind=jnp.bfloat16):
    drawn = jax.random.normal(stream_key, extent, jnp.float32) * spread
    return jnp.minimum(jnp.maximum(drawn, -most), most).astype(kind)


def setup_inputs(seed: int = 0) -> dict:
    key_of = jax.random.split(jax.random.key(seed), 6)
    tokens = draw_tokens(jax.random.fold_in(key_of[5], 71), 0)
    qkv_weight = scatter_about(key_of[1], (D, (QH + 2 * KVH) * HD), D ** -0.5, 0.09375)
    owner_slot = draw_owner_slot(jax.random.fold_in(key_of[5], 71), 0)
    slab_sequence = draw_slab_sequence(jax.random.fold_in(key_of[5], 71), 0)
    slab_order = draw_slab_order(jax.random.fold_in(key_of[5], 71), 0)
    return dict(tokens=tokens, qkv_weight=qkv_weight, owner_slot=owner_slot, slab_sequence=slab_sequence, slab_order=slab_order)


ROPE_BASE = 500000.0
NEG_FILL = -1e30


def rotate(heads, positions):
    half_dim = heads.shape[-1] // 2
    frequency = ROPE_BASE ** (-jnp.arange(half_dim, dtype=jnp.float32) * 2.0 / heads.shape[-1])
    angles = positions.astype(jnp.float32)[:, None] * frequency[None, :]
    cosine = jnp.cos(angles)[:, None, :]
    sine_part = jnp.sin(angles)[:, None, :]
    first_half = heads[..., :half_dim]
    second_half = heads[..., half_dim:]
    return jnp.concatenate([first_half * cosine - second_half * sine_part, second_half * cosine + first_half * sine_part], axis=-1)


def project(input_rows, weight, positions):
    projected = jnp.dot(input_rows, weight, preferred_element_type=jnp.float32)
    count_rows = input_rows.shape[0]
    query = rotate(projected[:, :QH * HD].reshape(count_rows, QH, HD), positions).astype(jnp.bfloat16)
    key_heads = rotate(projected[:, QH * HD:(QH + KVH) * HD].reshape(count_rows, KVH, HD), positions).astype(jnp.bfloat16)
    value_heads = projected[:, (QH + KVH) * HD:].astype(jnp.bfloat16)
    key_value = jnp.concatenate([key_heads.reshape(count_rows, KVH * HD), value_heads], axis=1)
    return query.reshape(count_rows, QH * HD), key_value


def attend(query, key_value, query_pos, query_code, key_code):
    count_rows = query.shape[0]
    block_rows = min(512, count_rows)
    group_size = QH // KVH
    keys_f = key_value[:, :KVH * HD].reshape(-1, KVH, HD).astype(jnp.float32)
    values_f = key_value[:, KVH * HD:].reshape(-1, KVH, HD).astype(jnp.float32)

    def per_block(args):
        query_block, pos_block, code_block = args
        query_f = query_block.reshape(block_rows, KVH, group_size, HD).astype(jnp.float32)
        scores = jnp.einsum('tgjh,ngh->gjtn', query_f, keys_f) * (HD ** -0.5)
        allowed = (key_code[None, :] <= code_block[:, None]) & (key_code[None, :] >= (code_block - pos_block)[:, None])
        scores = jnp.where(allowed, scores, NEG_FILL)
        row_max = jnp.max(scores, axis=-1, keepdims=True)
        weights = jnp.where(allowed, jnp.exp(scores - row_max), 0.0)
        denom_sum = jnp.sum(weights, axis=-1)
        rounded = lax.optimization_barrier(weights.astype(jnp.bfloat16))
        weighted = jnp.einsum('gjtn,ngh->gjth', rounded.astype(jnp.float32), values_f)
        context = weighted / denom_sum[..., None]
        return context.transpose(2, 0, 1, 3).reshape(block_rows, QH * HD).astype(jnp.bfloat16)

    blocks = count_rows // block_rows
    result = lax.map(per_block, (query.reshape(blocks, block_rows, QH * HD), query_pos.reshape(blocks, block_rows), query_code.reshape(blocks, block_rows)))
    return result.reshape(count_rows, QH * HD)


def reference(tokens, qkv_weight, owner_slot, slab_sequence, slab_order):
    columns_count = ROW_SLABS // SLABS_DEV
    slabs = tokens.reshape(GROUPS, columns_count, SLABS_DEV, SLAB, D)
    targets = owner_slot.reshape(GROUPS, columns_count, SLABS_DEV)
    columns = jnp.broadcast_to(jnp.arange(columns_count, dtype=jnp.int32)[None, :, None], targets.shape)
    owner_rows = jnp.zeros_like(slabs).at[targets // SLABS_DEV, columns, targets % SLABS_DEV].set(slabs)
    owner_rows = owner_rows.reshape(GROUPS, ROW_TOK, D)
    offsets = jnp.arange(SLAB, dtype=jnp.int32)
    positions = (slab_order[:, :, None] * SLAB + offsets[None, None, :]).reshape(GROUPS, ROW_TOK)
    codes = (slab_sequence[:, :, None] * ROW_TOK).reshape(GROUPS, ROW_SLABS, 1) + positions.reshape(GROUPS, ROW_SLABS, SLAB)
    codes = codes.reshape(GROUPS, ROW_TOK).astype(jnp.int32)

    def per_row(args):
        input_rows, row_pos, row_code = args
        query, key_value = project(input_rows, qkv_weight, row_pos)
        return attend(query, key_value, row_pos, row_code, row_code)

    return lax.map(per_row, (owner_rows, positions, codes))
```

```python
import functools
import math

import jax
import jax.numpy as jnp
import numpy as np
from jax import lax
from jax.experimental import pallas as pl
from jax.experimental.pallas import tpu as pltpu
from jax.sharding import PartitionSpec as P

QH = 16
KVH = 4
HD = 128
D = 4096
SLAB = 128
ROPE_BASE = 500000.0
NEG = 1e30
RING = 4
BF = jnp.bfloat16
F32 = jnp.float32
SCALE2 = HD ** (-0.5) * math.log2(math.e)


def rope_tables():
    freq = ROPE_BASE ** (-np.arange(64, dtype=np.float64) * 2.0 / HD)
    freq = np.concatenate([freq, freq])[None, :]
    sign = np.where(np.arange(HD) < 64, -1.0, 1.0)[None, :]
    low = np.arange(SLAB, dtype=np.float64)[:, None] * freq
    high = np.arange(16, dtype=np.float64)[:, None] * SLAB * freq
    table = np.concatenate([np.cos(low), np.sin(low) * sign, np.cos(high), np.sin(high) * sign])
    return table.astype(np.float32)


def kernel(
    own_ref, seq_ref, ord_ref, x_hbm, w_hbm, tab_hbm, out_ref,
    xv, wv, tab, kst, vst, qst, kx, vx, qx, kbuf, vbuf, flag, qsel, mst, lst, acc, ost,
    local_sem, send_sem, flag_sem, kx_sem, vx_sem, qx_sem, kg_sem, vg_sem, out_sem,
):
    row = lax.axis_index("dp")
    cp = lax.axis_index("cp")
    core = lax.rem(cp, 2)
    chip = cp // 2
    y = lax.rem(chip, RING)
    z = chip // RING
    other = 1 - core
    first = y * other + z * core
    second = z * other + y * core

    def cp_of(first_at, second_at, which_core):
        y_at = first_at * other + second_at * core
        z_at = second_at * other + first_at * core
        return (z_at * RING + y_at) * 2 + which_core

    def x_peer(shift, which_core):
        return (lax.rem(row + shift, RING), chip * 2 + which_core)

    def plane_peer(df, ds):
        return (row, cp_of(lax.rem(first + df, RING), lax.rem(second + ds, RING), core))

    def piece_col(df, ds):
        return cp_of(lax.rem(first + df, RING), lax.rem(second + ds, RING), 0)

    sends = []

    def send(src, dst, sem, peer):
        copy = pltpu.make_async_remote_copy(
            src_ref=src, dst_ref=dst, send_sem=send_sem.at[len(sends)], recv_sem=sem,
            device_id=peer, device_id_type=pl.DeviceIdType.MESH,
        )
        copy.start()
        sends.append(copy)

    def arrived(dst, sem):
        pltpu.make_async_remote_copy(
            src_ref=dst, dst_ref=dst, send_sem=send_sem.at[0], recv_sem=sem,
            device_id=(row, cp), device_id_type=pl.DeviceIdType.MESH,
        ).wait_recv()

    barrier = pltpu.get_barrier_semaphore()
    peers = [(row, chip * 2 + other)]
    for which in (0, 1):
        peers += [x_peer(shift, which) for shift in (1, 2, 3)]
    for shift in (1, 3):
        peers += [plane_peer(shift, 0), plane_peer(0, shift)]
    for peer in peers:
        pl.semaphore_signal(barrier, inc=1, device_id=peer, device_id_type=pl.DeviceIdType.MESH)

    columns = [2048, 2560, 0, 512, 1024, 1536]
    loads = [
        pltpu.make_async_copy(w_hbm.at[:, pl.ds(c, 512)], wv.at[i], local_sem.at[i])
        for i, c in enumerate(columns)
    ]
    x_load = pltpu.make_async_copy(x_hbm, xv, local_sem.at[6])
    tab_load = pltpu.make_async_copy(tab_hbm, tab, local_sem.at[7])
    x_load.start()
    tab_load.start()
    loads[0].start()
    loads[1].start()

    target = own_ref[0, 0]
    order = ord_ref[target, cp]
    flag[0, core] = jnp.full((8, 128), target, jnp.int32)
    tab_load.wait()
    cos_low, sin_low = tab[0:128, :], tab[128:256, :]
    cos_high = tab[pl.ds(256 + order, 1), :]
    sin_high = tab[pl.ds(272 + order, 1), :]
    cosine = cos_low * cos_high - sin_low * sin_high
    lane = lax.broadcasted_iota(jnp.int32, (SLAB, HD), 1)
    sign = jnp.where(lane < 64, -1.0, 1.0).astype(F32)
    sine = (sin_low * cos_high + cos_low * sin_high)

    def rope(head):
        return (head * cosine + pltpu.roll(head, 64, 1) * sine).astype(BF)

    def project(block):
        return jnp.dot(xv[...], wv[block], preferred_element_type=F32)

    x_load.wait()
    loads[0].wait()
    loads[2].start()
    loads[3].start()
    keys = project(0)
    for h in range(2):
        for g in range(2):
            c = (h * 2 + g) * HD
            kst[h, g] = rope(keys[:, c:c + HD])
    kx[0, core] = kst[core]
    pl.semaphore_wait(barrier, len(peers))

    send(flag.at[0, core], flag.at[0, core], flag_sem.at[0, 0], (row, chip * 2 + other))
    for shift in (1, 2, 3):
        back = RING - shift
        for which in (0, 1):
            send(flag.at[0, core], flag.at[back, core], flag_sem.at[back, core], x_peer(shift, which))

    def x_send(stage, xbuf, sem):
        for which in (0, 1):
            send(stage.at[which], xbuf.at[3, core], sem.at[3, core], x_peer(1, which))
            send(stage.at[which], xbuf.at[1, core], sem.at[1, core], x_peer(3, which))
        send(stage.at[other], xbuf.at[0, core], sem.at[0, 0], (row, chip * 2 + other))

    def x_relay(xbuf, sem):
        arrived(xbuf.at[3, 0], sem.at[3, 0])
        send(xbuf.at[3, 0], xbuf.at[2, 0], sem.at[2, 0], x_peer(1, core))
        arrived(xbuf.at[1, 1], sem.at[1, 1])
        send(xbuf.at[1, 1], xbuf.at[2, 1], sem.at[2, 1], x_peer(3, core))

    def x_rest(xbuf, sem):
        arrived(xbuf.at[0, other], sem.at[0, 0])
        arrived(xbuf.at[3, 1], sem.at[3, 1])
        arrived(xbuf.at[1, 0], sem.at[1, 0])
        arrived(xbuf.at[2, 0], sem.at[2, 0])
        arrived(xbuf.at[2, 1], sem.at[2, 1])

    x_send(kst, kx, kx_sem)
    loads[1].wait()
    loads[4].start()
    values = project(1)
    for h in range(2):
        for g in range(2):
            c = (h * 2 + g) * HD
            vst[h, g] = values[:, c:c + HD].T.astype(BF)
    vx[0, core] = vst[core]
    x_send(vst, vx, vx_sem)
    loads[2].wait()
    loads[5].start()

    def query_block(i):
        block = project(2 + i)
        for j in range(4):
            qst[i // 2, i % 2, :, j * HD:(j + 1) * HD] = rope(block[:, j * HD:(j + 1) * HD])

    query_block(0)
    loads[3].wait()
    query_block(1)
    x_relay(kx, kx_sem)
    loads[4].wait()
    query_block(2)
    x_relay(vx, vx_sem)
    loads[5].wait()
    query_block(3)
    qx[0, core] = qst[core]

    arrived(flag.at[0, other], flag_sem.at[0, 0])
    for d in (1, 2, 3):
        for p in (0, 1):
            arrived(flag.at[d, p], flag_sem.at[d, p])

    def pick(parts, p):
        total = None
        for d in range(RING):
            chosen = flag[d, p, 0:1, :] == row
            part = parts(d)
            wide = jnp.broadcast_to(chosen, part.shape)
            total = jnp.where(wide, part, jnp.zeros_like(part) if total is None else total)
        return total

    my_col = chip * 2

    def gather_start(xbuf, buf, sem, gsem):
        x_rest(xbuf, sem)
        for p in (0, 1):
            for g in (0, 1):
                buf[my_col + p, g] = pick(lambda d: xbuf[d, p, g], p)

    def hop(buf, gsem, df, ds, step_f, step_s, which=None):
        col = piece_col(df, ds)
        at = (df - step_f) % RING, (ds - step_s) % RING
        slot = buf.at[pl.ds(col, 2)] if which is None else buf.at[pl.ds(col + which, 1)]
        send(slot, slot, gsem.at[at[0], at[1], which or 0], plane_peer(step_f % RING, step_s % RING))

    def landed(buf, gsem, df, ds, which=None):
        col = piece_col(df, ds)
        slot = buf.at[pl.ds(col, 2)] if which is None else buf.at[pl.ds(col + which, 1)]
        arrived(slot, gsem.at[df, ds, which or 0])

    both = ((kbuf, kg_sem), (vbuf, vg_sem))
    for xbuf, sem, (buf, gsem) in ((kx, kx_sem, both[0]), (vx, vx_sem, both[1])):
        gather_start(xbuf, buf, sem, gsem)
        hop(buf, gsem, 0, 0, 1, 0)
        hop(buf, gsem, 0, 0, -1, 0)
        hop(buf, gsem, 0, 0, 0, 1)
        hop(buf, gsem, 0, 0, 0, -1)

    x_send(qst, qx, qx_sem)

    for buf, gsem in both:
        landed(buf, gsem, 3, 0)
        hop(buf, gsem, 3, 0, 1, 0, 0)
        hop(buf, gsem, 3, 0, 0, 1)
        hop(buf, gsem, 3, 0, 0, -1)
        landed(buf, gsem, 1, 0)
        hop(buf, gsem, 1, 0, -1, 0, 1)
        hop(buf, gsem, 1, 0, 0, 1)
        hop(buf, gsem, 1, 0, 0, -1)
    x_relay(qx, qx_sem)
    for buf, gsem in both:
        landed(buf, gsem, 2, 0, 0)
        landed(buf, gsem, 2, 0, 1)
        hop(buf, gsem, 2, 0, 0, 1)
        hop(buf, gsem, 2, 0, 0, -1)
    for df in (0, 3, 1, 2):
        for buf, gsem in both:
            landed(buf, gsem, df, 3)
            hop(buf, gsem, df, 3, 0, 1, 0)
            landed(buf, gsem, df, 1)
            hop(buf, gsem, df, 1, 0, -1, 1)
    for df in range(RING):
        for buf, gsem in both:
            landed(buf, gsem, df, 2, 0)
            landed(buf, gsem, df, 2, 1)

    x_rest(qx, qx_sem)
    for p in (0, 1):
        for g in (0, 1):
            for j in range(4):
                c = j * HD
                qsel[p * 2 + g, c:c + HD, :] = pick(lambda d: qx[d, p, g, :, c:c + HD], p)

    def penalty(p, col):
        same = seq_ref[row, my_col + p] == seq_ref[row, col]
        before = ord_ref[row, col] <= ord_ref[row, my_col + p]
        return jnp.where(jnp.logical_and(same, before), 0.0, NEG).astype(F32)

    def attend(col, p, g, diagonal):
        at = p * 2 + g
        query = qsel[at]
        key = jnp.concatenate([kbuf[col, g], kbuf[col + 1, g]], axis=0)
        scores = lax.dot_general(key, query, (((1,), (1,)), ((), ())), preferred_element_type=F32)
        halves = [scores[:SLAB], scores[SLAB:]]
        shift = [penalty(p, col), penalty(p, col + 1)]
        if diagonal:
            key_at = lax.broadcasted_iota(jnp.int32, (SLAB, 4 * SLAB), 0)
            query_at = lax.rem(lax.broadcasted_iota(jnp.int32, (SLAB, 4 * SLAB), 1), SLAB)
            halves[p] = jnp.where(key_at <= query_at, halves[p], -NEG)
        peak = jnp.maximum(
            jnp.max(halves[0], axis=0, keepdims=True) - shift[0],
            jnp.max(halves[1], axis=0, keepdims=True) - shift[1],
        )
        if not diagonal:
            old = mst[at]
            peak = jnp.maximum(peak, old)
        base = peak * SCALE2
        weights = [jnp.exp2(halves[i] * SCALE2 - (base + shift[i])) for i in (0, 1)]
        total = jnp.sum(weights[0], axis=0, keepdims=True) + jnp.sum(weights[1], axis=0, keepdims=True)
        rounded = jnp.concatenate([w.astype(BF) for w in weights], axis=0)
        value = jnp.concatenate([vbuf[col, g], vbuf[col + 1, g]], axis=1)
        product = jnp.dot(value, rounded, preferred_element_type=F32)
        mst[at] = peak
        if diagonal:
            lst[at] = total
            acc[at] = product
        else:
            fade = jnp.exp2((old - peak) * SCALE2)
            lst[at] = lst[at] * fade + total
            acc[at] = acc[at] * fade + product

    for p in (0, 1):
        for g in (0, 1):
            attend(my_col, p, g, True)

    def step(i, carry):
        col = cp_of(lax.rem(first + lax.rem(i, RING), RING), lax.rem(second + i // RING, RING), 0)
        for p in (0, 1):
            for g in (0, 1):
                attend(col, p, g, False)
        return carry

    lax.fori_loop(1, RING * RING, step, 0)

    def finish(p, g):
        at = p * 2 + g
        result = acc[at] / lst[at]
        return [result[:, j * HD:(j + 1) * HD].T.astype(BF) for j in range(4)]

    for g in (0, 1):
        for j, part in enumerate(finish(other, g)):
            ost[:, (g * 4 + j) * HD:(g * 4 + j + 1) * HD] = part
    send(ost, out_ref.at[core], out_sem.at[0], (row, chip * 2 + other))
    for g in (0, 1):
        for j, part in enumerate(finish(core, g)):
            out_ref[core, :, (g * 4 + j) * HD:(g * 4 + j + 1) * HD] = part
    arrived(out_ref.at[other], out_sem.at[0])
    for copy in sends:
        copy.wait_send()


def local(tokens, qkv_weight, owner_slot, slab_sequence, slab_order):
    smem = pl.BlockSpec(memory_space=pltpu.SMEM)
    hbm = pl.BlockSpec(memory_space=pl.ANY)
    dma = pltpu.SemaphoreType.DMA
    out = pl.pallas_call(
        kernel,
        out_shape=jax.ShapeDtypeStruct((2, SLAB, QH * HD // 2), BF),
        in_specs=[smem, smem, smem, hbm, hbm, hbm],
        out_specs=pl.BlockSpec(memory_space=pltpu.VMEM),
        scratch_shapes=[
            pltpu.VMEM((SLAB, D), BF),
            pltpu.VMEM((6, D, 512), BF),
            pltpu.VMEM((288, HD), F32),
            pltpu.VMEM((2, 2, SLAB, HD), BF),
            pltpu.VMEM((2, 2, HD, SLAB), BF),
            pltpu.VMEM((2, 2, SLAB, 512), BF),
            pltpu.VMEM((4, 2, 2, SLAB, HD), BF),
            pltpu.VMEM((4, 2, 2, HD, SLAB), BF),
            pltpu.VMEM((4, 2, 2, SLAB, 512), BF),
            pltpu.VMEM((32, 2, SLAB, HD), BF),
            pltpu.VMEM((32, 2, HD, SLAB), BF),
            pltpu.VMEM((4, 2, 8, 128), jnp.int32),
            pltpu.VMEM((4, 512, HD), BF),
            pltpu.VMEM((4, 1, 512), F32),
            pltpu.VMEM((4, 1, 512), F32),
            pltpu.VMEM((4, HD, 512), F32),
            pltpu.VMEM((SLAB, 1024), BF),
            dma((8,)),
            dma((80,)),
            dma((4, 2)),
            dma((4, 2)),
            dma((4, 2)),
            dma((4, 2)),
            dma((4, 4, 2)),
            dma((4, 4, 2)),
            dma((1,)),
        ],
        compiler_params=pltpu.CompilerParams(
            collective_id=0, has_side_effects=True, vmem_limit_bytes=62 * 1024 * 1024
        ),
        name="slab_attention",
    )(owner_slot, slab_sequence, slab_order, tokens[0], qkv_weight, jnp.asarray(rope_tables()))
    return out.transpose(1, 0, 2).reshape(1, SLAB, QH * HD)


def solution(mesh):
    in_specs = (P("dp", "cp", None), P(), P("dp", "cp"), P(), P())
    out_specs = P("dp", "cp", None)
    return jax.shard_map(local, mesh=mesh, in_specs=in_specs, out_specs=out_specs, check_vma=False)
```

```python
import functools
import math

import jax
import jax.numpy as jnp
import numpy as np
from jax import lax
from jax.experimental import pallas as pl
from jax.experimental.pallas import tpu as pltpu
from jax.sharding import PartitionSpec as P

QH = 16
KVH = 4
HD = 128
D = 4096
SLAB = 128
ROPE_BASE = 500000.0
NEG = 1e30
RING = 4
BF = jnp.bfloat16
F32 = jnp.float32
SCALE2 = HD ** (-0.5) * math.log2(math.e)


def rope_tables():
    freq = ROPE_BASE ** (-np.arange(64, dtype=np.float64) * 2.0 / HD)
    freq = np.concatenate([freq, freq])[None, :]
    sign = np.where(np.arange(HD) < 64, -1.0, 1.0)[None, :]
    low = np.arange(SLAB, dtype=np.float64)[:, None] * freq
    high = np.arange(16, dtype=np.float64)[:, None] * SLAB * freq
    table = np.concatenate([np.cos(low), np.sin(low) * sign, np.cos(high), np.sin(high) * sign])
    return table.astype(np.float32)


def kernel(
    own_ref, seq_ref, ord_ref, x_hbm, w_hbm, tab_hbm, out_ref,
    xv, wv, tab, kst, vst, qst, kx, vx, qx, kbuf, vbuf, flag, qsel, sbuf, ost, code_ref, pick_ref,
    local_sem, send_sem, flag_sem, kx_sem, vx_sem, qx_sem, kg_sem, vg_sem, out_sem,
):
    row = lax.axis_index("dp")
    cp = lax.axis_index("cp")
    core = lax.rem(cp, 2)
    chip = cp // 2
    y = lax.rem(chip, RING)
    z = chip // RING
    other = 1 - core
    first = y * other + z * core
    second = z * other + y * core

    def cp_of(first_at, second_at, which_core):
        y_at = first_at * other + second_at * core
        z_at = second_at * other + first_at * core
        return (z_at * RING + y_at) * 2 + which_core

    def x_peer(shift, which_core):
        return (lax.rem(row + shift, RING), chip * 2 + which_core)

    def plane_peer(df, ds):
        return (row, cp_of(lax.rem(first + df, RING), lax.rem(second + ds, RING), core))

    def piece_col(df, ds):
        return cp_of(lax.rem(first + df, RING), lax.rem(second + ds, RING), 0)

    sends = []

    def send(src, dst, sem, peer):
        copy = pltpu.make_async_remote_copy(
            src_ref=src, dst_ref=dst, send_sem=send_sem.at[len(sends)], recv_sem=sem,
            device_id=peer, device_id_type=pl.DeviceIdType.MESH,
        )
        copy.start()
        sends.append(copy)

    def arrived(dst, sem):
        pltpu.make_async_remote_copy(
            src_ref=dst, dst_ref=dst, send_sem=send_sem.at[0], recv_sem=sem,
            device_id=(row, cp), device_id_type=pl.DeviceIdType.MESH,
        ).wait_recv()

    barrier = pltpu.get_barrier_semaphore()
    peers = [(row, chip * 2 + other)]
    for which in (0, 1):
        peers += [x_peer(shift, which) for shift in (1, 2, 3)]
    for shift in (1, 3):
        peers += [plane_peer(shift, 0), plane_peer(0, shift)]
    for peer in peers:
        pl.semaphore_signal(barrier, inc=1, device_id=peer, device_id_type=pl.DeviceIdType.MESH)

    columns = [2048, 2560, 0, 512, 1024, 1536]
    loads = [
        pltpu.make_async_copy(w_hbm.at[:, pl.ds(c, 512)], wv.at[i], local_sem.at[i])
        for i, c in enumerate(columns)
    ]
    x_load = pltpu.make_async_copy(x_hbm, xv, local_sem.at[6])
    tab_load = pltpu.make_async_copy(tab_hbm, tab, local_sem.at[7])
    x_load.start()
    tab_load.start()
    loads[0].start()
    loads[1].start()

    target = own_ref[0, 0]
    order = ord_ref[target, cp]
    flag[0, core] = jnp.full((8, 128), target, jnp.int32)
    tab_load.wait()
    cos_low, sin_low = tab[0:128, :], tab[128:256, :]
    cos_high = tab[pl.ds(256 + order, 1), :]
    sin_high = tab[pl.ds(272 + order, 1), :]
    cosine = cos_low * cos_high - sin_low * sin_high
    sine = sin_low * cos_high + cos_low * sin_high

    def rope(head):
        return (head * cosine + pltpu.roll(head, 64, 1) * sine).astype(BF)

    def project(block):
        return jnp.dot(xv[...], wv[block], preferred_element_type=F32)

    x_load.wait()
    loads[0].wait()
    loads[2].start()
    loads[3].start()
    keys = project(0)
    for h in range(2):
        for g in range(2):
            c = (h * 2 + g) * HD
            kst[h, g] = rope(keys[:, c:c + HD])
    kx[0, core] = kst[core]
    pl.semaphore_wait(barrier, len(peers))

    send(flag.at[0, core], flag.at[0, core], flag_sem.at[0, 0], (row, chip * 2 + other))
    for shift in (1, 2, 3):
        back = RING - shift
        for which in (0, 1):
            send(flag.at[0, core], flag.at[back, core], flag_sem.at[back, core], x_peer(shift, which))

    def x_send(stage, xbuf, sem):
        for which in (0, 1):
            send(stage.at[which], xbuf.at[3, core], sem.at[3, core], x_peer(1, which))
            send(stage.at[which], xbuf.at[1, core], sem.at[1, core], x_peer(3, which))
        send(stage.at[other], xbuf.at[0, core], sem.at[0, 0], (row, chip * 2 + other))

    def x_relay(xbuf, sem):
        arrived(xbuf.at[3, 0], sem.at[3, 0])
        send(xbuf.at[3, 0], xbuf.at[2, 0], sem.at[2, 0], x_peer(1, core))
        arrived(xbuf.at[1, 1], sem.at[1, 1])
        send(xbuf.at[1, 1], xbuf.at[2, 1], sem.at[2, 1], x_peer(3, core))

    def x_rest(xbuf, sem):
        arrived(xbuf.at[0, other], sem.at[0, 0])
        arrived(xbuf.at[3, 1], sem.at[3, 1])
        arrived(xbuf.at[1, 0], sem.at[1, 0])
        arrived(xbuf.at[2, 0], sem.at[2, 0])
        arrived(xbuf.at[2, 1], sem.at[2, 1])

    x_send(kst, kx, kx_sem)
    loads[1].wait()
    loads[4].start()
    values = project(1)
    for h in range(2):
        for g in range(2):
            c = (h * 2 + g) * HD
            vst[h, g] = values[:, c:c + HD].T.astype(BF)
    vx[0, core] = vst[core]
    x_send(vst, vx, vx_sem)
    loads[2].wait()
    loads[5].start()

    def query_block(i):
        block = project(2 + i)
        for j in range(4):
            qst[i // 2, i % 2, :, j * HD:(j + 1) * HD] = rope(block[:, j * HD:(j + 1) * HD])

    query_block(0)
    loads[3].wait()
    query_block(1)
    my_col = chip * 2
    for j in range(32):
        code_ref[j] = seq_ref[row, j] * 16 + ord_ref[row, j]

    def look_up(i, carry):
        wanted = seq_ref[row, my_col + i // 16] * 16 + lax.rem(i, 16)
        found = 0
        for j in range(32):
            found = jnp.where(code_ref[j] == wanted, j, found)
        pick_ref[i // 16, lax.rem(i, 16)] = found
        return carry

    lax.fori_loop(0, 32, look_up, 0)
    x_relay(kx, kx_sem)
    loads[4].wait()
    query_block(2)
    x_relay(vx, vx_sem)
    loads[5].wait()
    query_block(3)
    qx[0, core] = qst[core]

    arrived(flag.at[0, other], flag_sem.at[0, 0])
    for d in (1, 2, 3):
        for p in (0, 1):
            arrived(flag.at[d, p], flag_sem.at[d, p])

    def pick(parts, p):
        total = None
        for d in range(RING):
            chosen = flag[d, p, 0:1, :] == row
            part = parts(d)
            wide = jnp.broadcast_to(chosen, part.shape)
            total = jnp.where(wide, part, jnp.zeros_like(part) if total is None else total)
        return total

    def gather_start(xbuf, buf, sem, gsem):
        x_rest(xbuf, sem)
        for p in (0, 1):
            for g in (0, 1):
                buf[my_col + p, g] = pick(lambda d: xbuf[d, p, g], p)

    def hop(buf, gsem, df, ds, step_f, step_s, which=None):
        col = piece_col(df, ds)
        at = (df - step_f) % RING, (ds - step_s) % RING
        slot = buf.at[pl.ds(col, 2)] if which is None else buf.at[pl.ds(col + which, 1)]
        send(slot, slot, gsem.at[at[0], at[1], which or 0], plane_peer(step_f % RING, step_s % RING))

    def landed(buf, gsem, df, ds, which=None):
        col = piece_col(df, ds)
        slot = buf.at[pl.ds(col, 2)] if which is None else buf.at[pl.ds(col + which, 1)]
        arrived(slot, gsem.at[df, ds, which or 0])

    both = ((kbuf, kg_sem), (vbuf, vg_sem))
    for xbuf, sem, (buf, gsem) in ((kx, kx_sem, both[0]), (vx, vx_sem, both[1])):
        gather_start(xbuf, buf, sem, gsem)
        hop(buf, gsem, 0, 0, 1, 0)
        hop(buf, gsem, 0, 0, -1, 0)
        hop(buf, gsem, 0, 0, 0, 1)
        hop(buf, gsem, 0, 0, 0, -1)

    x_send(qst, qx, qx_sem)

    for buf, gsem in both:
        landed(buf, gsem, 3, 0)
        hop(buf, gsem, 3, 0, 1, 0, 0)
        hop(buf, gsem, 3, 0, 0, 1)
        hop(buf, gsem, 3, 0, 0, -1)
        landed(buf, gsem, 1, 0)
        hop(buf, gsem, 1, 0, -1, 0, 1)
        hop(buf, gsem, 1, 0, 0, 1)
        hop(buf, gsem, 1, 0, 0, -1)
    x_relay(qx, qx_sem)
    for buf, gsem in both:
        landed(buf, gsem, 2, 0, 0)
        landed(buf, gsem, 2, 0, 1)
        hop(buf, gsem, 2, 0, 0, 1)
        hop(buf, gsem, 2, 0, 0, -1)
    for df in (0, 3, 1, 2):
        for buf, gsem in both:
            landed(buf, gsem, df, 3)
            hop(buf, gsem, df, 3, 0, 1, 0)
            landed(buf, gsem, df, 1)
            hop(buf, gsem, df, 1, 0, -1, 1)
    for df in range(RING):
        for buf, gsem in both:
            landed(buf, gsem, df, 2, 0)
            landed(buf, gsem, df, 2, 1)

    x_rest(qx, qx_sem)
    for p in (0, 1):
        for g in (0, 1):
            for j in range(4):
                c = j * HD
                qsel[p * 2 + g, c:c + HD, :] = pick(lambda d: qx[d, p, g, :, c:c + HD], p)

    def scores_of(t, p, g, own, query):
        if t == 0:
            cols = (my_col + p, pick_ref[p, 14])
            later = (0.0, jnp.where(own > 14, 0.0, NEG).astype(F32))
        else:
            cols = (pick_ref[p, 2 * t - 2], pick_ref[p, 2 * t - 1])
            later = tuple(jnp.where(own > o, 0.0, NEG).astype(F32) for o in (2 * t - 2, 2 * t - 1))
        key = jnp.concatenate([kbuf[cols[0], g], kbuf[cols[1], g]], axis=0)
        scores = lax.dot_general(key, query, (((1,), (1,)), ((), ())), preferred_element_type=F32)
        halves = [scores[:SLAB], scores[SLAB:]]
        if t == 0:
            key_at = lax.broadcasted_iota(jnp.int32, (SLAB, 4 * SLAB), 0)
            query_at = lax.rem(lax.broadcasted_iota(jnp.int32, (SLAB, 4 * SLAB), 1), SLAB)
            halves[0] = jnp.where(key_at <= query_at, halves[0], -NEG)
        return cols, later, halves

    def attend(p, g):
        own = ord_ref[row, my_col + p]
        query = qsel[p * 2 + g]
        peak = None
        steps = []
        for t in range(8):
            cols, later, halves = scores_of(t, p, g, own, query)
            for i in (0, 1):
                sbuf[t, i] = halves[i]
                top = jnp.max(halves[i].reshape(16, 8, 512), axis=0) - later[i]
                peak = top if peak is None else jnp.maximum(peak, top)
            steps.append((cols, later))
        base = jnp.max(peak, axis=0, keepdims=True) * SCALE2
        total, product = None, None
        for t in range(8):
            cols, later = steps[t]
            parts = []
            for i in (0, 1):
                weight = jnp.exp2(sbuf[t, i] * SCALE2 - (base + later[i]))
                part = jnp.sum(weight.reshape(16, 8, 512), axis=0)
                total = part if total is None else total + part
                parts.append(weight.astype(BF))
            value = jnp.concatenate([vbuf[cols[0], g], vbuf[cols[1], g]], axis=1)
            term = jnp.dot(value, jnp.concatenate(parts, axis=0), preferred_element_type=F32)
            product = term if product is None else product + term
        result = product / jnp.sum(total, axis=0, keepdims=True)
        return [result[:, j * HD:(j + 1) * HD].T.astype(BF) for j in range(4)]

    def other_side(g, carry):
        for j, part in enumerate(attend(other, g)):
            ost[g, :, j * HD:(j + 1) * HD] = part
        return carry

    lax.fori_loop(0, 2, other_side, 0)
    for g in (0, 1):
        there = out_ref.at[:, pl.ds(pl.multiple_of(core * 1024 + g * 512, 512), 512)]
        send(ost.at[g], there, out_sem.at[g], (row, chip * 2 + other))

    def own_side(g, carry):
        parts = attend(core, g)
        out_ref[:, pl.ds(pl.multiple_of(core * 1024 + g * 512, 512), 512)] = jnp.concatenate(parts, axis=1)
        return carry

    lax.fori_loop(0, 2, own_side, 0)
    for g in (0, 1):
        here = out_ref.at[:, pl.ds(pl.multiple_of(other * 1024 + g * 512, 512), 512)]
        arrived(here, out_sem.at[g])
    for copy in sends:
        copy.wait_send()


def local(tokens, qkv_weight, owner_slot, slab_sequence, slab_order):
    smem = pl.BlockSpec(memory_space=pltpu.SMEM)
    hbm = pl.BlockSpec(memory_space=pl.ANY)
    dma = pltpu.SemaphoreType.DMA
    out = pl.pallas_call(
        kernel,
        out_shape=jax.ShapeDtypeStruct((SLAB, QH * HD), BF),
        in_specs=[smem, smem, smem, hbm, hbm, hbm],
        out_specs=pl.BlockSpec(memory_space=pltpu.VMEM),
        scratch_shapes=[
            pltpu.VMEM((SLAB, D), BF),
            pltpu.VMEM((6, D, 512), BF),
            pltpu.VMEM((288, HD), F32),
            pltpu.VMEM((2, 2, SLAB, HD), BF),
            pltpu.VMEM((2, 2, HD, SLAB), BF),
            pltpu.VMEM((2, 2, SLAB, 512), BF),
            pltpu.VMEM((4, 2, 2, SLAB, HD), BF),
            pltpu.VMEM((4, 2, 2, HD, SLAB), BF),
            pltpu.VMEM((4, 2, 2, SLAB, 512), BF),
            pltpu.VMEM((32, 2, SLAB, HD), BF),
            pltpu.VMEM((32, 2, HD, SLAB), BF),
            pltpu.VMEM((4, 2, 8, 128), jnp.int32),
            pltpu.VMEM((4, 512, HD), BF),
            pltpu.VMEM((8, 2, SLAB, 512), F32),
            pltpu.VMEM((2, SLAB, 512), BF),
            pltpu.SMEM((32,), jnp.int32),
            pltpu.SMEM((2, 16), jnp.int32),
            dma((8,)),
            dma((80,)),
            dma((4, 2)),
            dma((4, 2)),
            dma((4, 2)),
            dma((4, 2)),
            dma((4, 4, 2)),
            dma((4, 4, 2)),
            dma((2,)),
        ],
        compiler_params=pltpu.CompilerParams(
            collective_id=0, has_side_effects=True, vmem_limit_bytes=62 * 1024 * 1024
        ),
        name="slab_attention",
    )(owner_slot, slab_sequence, slab_order, tokens[0], qkv_weight, jnp.asarray(rope_tables()))
    return out[None]


def solution(mesh):
    in_specs = (P("dp", "cp", None), P(), P("dp", "cp"), P(), P())
    out_specs = P("dp", "cp", None)
    return jax.shard_map(local, mesh=mesh, in_specs=in_specs, out_specs=out_specs, check_vma=False)
```

```python
import functools
import math

import jax
import jax.numpy as jnp
import numpy as np
from jax import lax
from jax.experimental import pallas as pl
from jax.experimental.pallas import tpu as pltpu
from jax.sharding import PartitionSpec as P

QH = 16
KVH = 4
HD = 128
D = 4096
SLAB = 128
ROPE_BASE = 500000.0
NEG = 1e30
RING = 4
BF = jnp.bfloat16
F32 = jnp.float32
SCALE2 = HD ** (-0.5) * math.log2(math.e)


def rope_tables():
    freq = ROPE_BASE ** (-np.arange(64, dtype=np.float64) * 2.0 / HD)
    freq = np.concatenate([freq, freq])[None, :]
    sign = np.where(np.arange(HD) < 64, -1.0, 1.0)[None, :]
    low = np.arange(SLAB, dtype=np.float64)[:, None] * freq
    high = np.arange(16, dtype=np.float64)[:, None] * SLAB * freq
    table = np.concatenate([np.cos(low), np.sin(low) * sign, np.cos(high), np.sin(high) * sign])
    return table.astype(np.float32)


def kernel(
    own_ref, seq_hbm, ord_hbm, x_hbm, w_hbm, tab_hbm, out_ref,
    seq_ref, ord_ref,
    xv, wv, tab, kst, vst, qst, kx, vx, qx, kbuf0, kbuf1, vbuf0, vbuf1, flag, qsel, sbuf, mbuf, ost, code_ref, pick_ref,
    local_sem, send_sem, flag_sem, kx_sem, vx_sem, qx_sem, kg_sem, vg_sem, out_sem,
):
    row = lax.axis_index("dp")
    cp = lax.axis_index("cp")
    core = lax.rem(cp, 2)
    chip = cp // 2
    y = lax.rem(chip, RING)
    z = chip // RING
    other = 1 - core
    first = y * other + z * core
    second = z * other + y * core

    def cp_of(first_at, second_at, which_core):
        y_at = first_at * other + second_at * core
        z_at = second_at * other + first_at * core
        return (z_at * RING + y_at) * 2 + which_core

    def x_peer(shift, which_core):
        return (lax.rem(row + shift, RING), chip * 2 + which_core)

    def plane_peer(df, ds):
        return (row, cp_of(lax.rem(first + df, RING), lax.rem(second + ds, RING), core))

    def piece_col(df, ds):
        return cp_of(lax.rem(first + df, RING), lax.rem(second + ds, RING), 0)

    sends = []

    def send(src, dst, sem, peer):
        copy = pltpu.make_async_remote_copy(
            src_ref=src, dst_ref=dst, send_sem=send_sem.at[len(sends)], recv_sem=sem,
            device_id=peer, device_id_type=pl.DeviceIdType.MESH,
        )
        copy.start()
        sends.append(copy)

    def arrived(dst, sem):
        pltpu.make_async_remote_copy(
            src_ref=dst, dst_ref=dst, send_sem=send_sem.at[0], recv_sem=sem,
            device_id=(row, cp), device_id_type=pl.DeviceIdType.MESH,
        ).wait_recv()

    columns = [2048, 2560, 0, 512, 1024, 1536]
    loads = [
        pltpu.make_async_copy(w_hbm.at[:, pl.ds(c, 512)], wv.at[i], local_sem.at[i])
        for i, c in enumerate(columns)
    ]
    x_load = pltpu.make_async_copy(x_hbm, xv, local_sem.at[6])
    tab_load = pltpu.make_async_copy(tab_hbm, tab, local_sem.at[7])
    small = [
        pltpu.make_async_copy(src, dst, local_sem.at[8 + i])
        for i, (src, dst) in enumerate(((seq_hbm, seq_ref), (ord_hbm, ord_ref)))
    ]
    for copy in small:
        copy.start()
    x_load.start()
    loads[0].start()
    tab_load.start()
    loads[1].start()

    barrier = pltpu.get_barrier_semaphore()
    peers = [(row, chip * 2 + other)]
    for which in (0, 1):
        peers += [x_peer(shift, which) for shift in (1, 2, 3)]
    for shift in (1, 3):
        peers += [plane_peer(shift, 0), plane_peer(0, shift)]
    for peer in peers:
        pl.semaphore_signal(barrier, inc=1, device_id=peer, device_id_type=pl.DeviceIdType.MESH)

    for copy in small:
        copy.wait()
    target = own_ref[0, 0]
    order = ord_ref[target, cp]
    flag[0, core] = jnp.full((8, 128), target, jnp.int32)
    tab_load.wait()
    cos_low, sin_low = tab[0:128, :], tab[128:256, :]
    cos_high = tab[pl.ds(256 + order, 1), :]
    sin_high = tab[pl.ds(272 + order, 1), :]
    cosine = cos_low * cos_high - sin_low * sin_high
    sine = sin_low * cos_high + cos_low * sin_high

    def rope(head):
        return (head * cosine + pltpu.roll(head, 64, 1) * sine).astype(BF)

    def project(block):
        return jnp.dot(xv[...], wv[block], preferred_element_type=F32)

    x_load.wait()
    loads[0].wait()
    loads[2].start()
    loads[3].start()
    keys = project(0)
    for h in range(2):
        for g in range(2):
            c = (h * 2 + g) * HD
            kst[h, g] = rope(keys[:, c:c + HD])
    kx[0, core] = kst[core]
    pl.semaphore_wait(barrier, len(peers))

    send(flag.at[0, core], flag.at[0, core], flag_sem.at[0, 0], (row, chip * 2 + other))
    for shift in (1, 2, 3):
        back = RING - shift
        for which in (0, 1):
            send(flag.at[0, core], flag.at[back, core], flag_sem.at[back, core], x_peer(shift, which))

    def x_send(stage, xbuf, sem, g, halves=(0, 1)):
        for which in halves:
            send(stage.at[which, g], xbuf.at[3, core, g], sem.at[g, 3, core], x_peer(1, which))
            send(stage.at[which, g], xbuf.at[1, core, g], sem.at[g, 1, core], x_peer(3, which))
        if 0 in halves:
            send(stage.at[other, g], xbuf.at[0, core, g], sem.at[g, 0, 0], (row, chip * 2 + other))

    def x_relay(xbuf, sem, g):
        arrived(xbuf.at[3, 0, g], sem.at[g, 3, 0])
        send(xbuf.at[3, 0, g], xbuf.at[2, 0, g], sem.at[g, 2, 0], x_peer(1, core))
        arrived(xbuf.at[1, 1, g], sem.at[g, 1, 1])
        send(xbuf.at[1, 1, g], xbuf.at[2, 1, g], sem.at[g, 2, 1], x_peer(3, core))

    def x_rest(xbuf, sem, g):
        arrived(xbuf.at[0, other, g], sem.at[g, 0, 0])
        arrived(xbuf.at[3, 1, g], sem.at[g, 3, 1])
        arrived(xbuf.at[1, 0, g], sem.at[g, 1, 0])
        arrived(xbuf.at[2, 0, g], sem.at[g, 2, 0])
        arrived(xbuf.at[2, 1, g], sem.at[g, 2, 1])

    my_col = chip * 2
    kbuf, vbuf = (kbuf0, kbuf1), (vbuf0, vbuf1)

    def query_block(i):
        block = project(2 + i)
        for j in range(4):
            qst[i // 2, i % 2, :, j * HD:(j + 1) * HD] = rope(block[:, j * HD:(j + 1) * HD])

    def look_up(i, carry):
        wanted = seq_ref[row, my_col + i // 16] * 16 + lax.rem(i, 16)
        found = 0
        for j in range(32):
            found = jnp.where(code_ref[j] == wanted, j, found)
        pick_ref[i // 16, lax.rem(i, 16)] = found
        return carry

    def flags_arrived():
        arrived(flag.at[0, other], flag_sem.at[0, 0])
        for d in (1, 2, 3):
            for p in (0, 1):
                arrived(flag.at[d, p], flag_sem.at[d, p])

    def pick(parts, p):
        total = None
        for d in range(RING):
            chosen = flag[d, p, 0:1, :] == row
            part = parts(d)
            wide = jnp.broadcast_to(chosen, part.shape)
            total = jnp.where(wide, part, jnp.zeros_like(part) if total is None else total)
        return total

    chunks = [(kx, kx_sem, kbuf, kg_sem, 0), (vx, vx_sem, vbuf, vg_sem, 0),
              (kx, kx_sem, kbuf, kg_sem, 1), (vx, vx_sem, vbuf, vg_sem, 1)]

    def slot_of(buf, g, df, ds, which):
        col = piece_col(df, ds)
        return buf[g].at[pl.ds(col, 2)] if which is None else buf[g].at[pl.ds(col + which, 1)]

    def hop(chunk, df, ds, step_f, step_s, which=None):
        _, _, buf, gsem, g = chunk
        at = (df - step_f) % RING, (ds - step_s) % RING
        slot = slot_of(buf, g, df, ds, which)
        send(slot, slot, gsem.at[g, at[0], at[1], which or 0], plane_peer(step_f % RING, step_s % RING))

    def landed(chunk, df, ds, which=None):
        _, _, buf, gsem, g = chunk
        arrived(slot_of(buf, g, df, ds, which), gsem.at[g, df, ds, which or 0])

    def begin(chunk):
        xbuf, sem, buf, gsem, g = chunk
        x_rest(xbuf, sem, g)
        for p in (0, 1):
            buf[g][my_col + p] = pick(lambda d: xbuf[d, p, g], p)
        hop(chunk, 0, 0, 1, 0)
        hop(chunk, 0, 0, -1, 0)
        hop(chunk, 0, 0, 0, 1)
        hop(chunk, 0, 0, 0, -1)

    def near(chunk):
        landed(chunk, 3, 0)
        hop(chunk, 3, 0, 1, 0, 0)
        hop(chunk, 3, 0, 0, 1)
        hop(chunk, 3, 0, 0, -1)
        landed(chunk, 1, 0)
        hop(chunk, 1, 0, -1, 0, 1)
        hop(chunk, 1, 0, 0, 1)
        hop(chunk, 1, 0, 0, -1)

    def far(chunk):
        landed(chunk, 2, 0, 0)
        landed(chunk, 2, 0, 1)
        hop(chunk, 2, 0, 0, 1)
        hop(chunk, 2, 0, 0, -1)

    def cross(chunk):
        for df in (0, 3, 1, 2):
            landed(chunk, df, 3)
            hop(chunk, df, 3, 0, 1, 0)
            landed(chunk, df, 1)
            hop(chunk, df, 1, 0, -1, 1)

    def last(chunk):
        for df in range(RING):
            landed(chunk, df, 2, 0)
            landed(chunk, df, 2, 1)

    def slabs_of(t, p, own):
        if t == 0:
            cols = (my_col + p, pick_ref[p, 14])
            later = (0.0, jnp.where(own > 14, 0.0, NEG).astype(F32))
        else:
            cols = (pick_ref[p, 2 * t - 2], pick_ref[p, 2 * t - 1])
            later = tuple(jnp.where(own > o, 0.0, NEG).astype(F32) for o in (2 * t - 2, 2 * t - 1))
        return cols, later

    def scores_of(t, p, g, own, query):
        cols, later = slabs_of(t, p, own)
        key = jnp.concatenate([kbuf[g][cols[0]], kbuf[g][cols[1]]], axis=0)
        scores = lax.dot_general(key, query, (((1,), (1,)), ((), ())), preferred_element_type=F32)
        halves = [scores[:SLAB], scores[SLAB:]]
        if t == 0:
            key_at = lax.broadcasted_iota(jnp.int32, (SLAB, 4 * SLAB), 0)
            query_at = lax.rem(lax.broadcasted_iota(jnp.int32, (SLAB, 4 * SLAB), 1), SLAB)
            halves[0] = jnp.where(key_at <= query_at, halves[0], -NEG)
        return cols, later, halves

    def first_pass(p, g, at):
        own = ord_ref[row, my_col + p]
        query = qsel[p * 2 + g]
        peak = None
        for t in range(8):
            cols, later, halves = scores_of(t, p, g, own, query)
            for i in (0, 1):
                sbuf[at, t, i] = halves[i]
                top = jnp.max(halves[i].reshape(16, 8, 512), axis=0) - later[i]
                peak = top if peak is None else jnp.maximum(peak, top)
        mbuf[at] = jnp.max(peak, axis=0, keepdims=True) * SCALE2

    def second_pass(p, g, at):
        own = ord_ref[row, my_col + p]
        base = mbuf[at]
        total, product = None, None
        for t in range(8):
            cols, later = slabs_of(t, p, own)
            parts = []
            for i in (0, 1):
                weight = jnp.exp2(sbuf[at, t, i] * SCALE2 - (base + later[i]))
                part = jnp.sum(weight.reshape(16, 8, 512), axis=0)
                total = part if total is None else total + part
                parts.append(weight.astype(BF))
            value = jnp.concatenate([vbuf[g][cols[0]], vbuf[g][cols[1]]], axis=1)
            term = jnp.dot(value, jnp.concatenate(parts, axis=0), preferred_element_type=F32)
            product = term if product is None else product + term
        result = product / jnp.sum(total, axis=0, keepdims=True)
        return jnp.concatenate([result[:, j * HD:(j + 1) * HD].T.astype(BF) for j in range(4)], axis=1)

    def columns_of(half, g):
        return pl.ds(pl.multiple_of(half * 1024 + g * 512, 512), 512)

    def give(g):
        ost[g] = second_pass(other, g, 0)
        send(ost.at[g], out_ref.at[:, columns_of(core, g)], out_sem.at[g], (row, chip * 2 + other))

    def keep(g):
        out_ref[:, columns_of(core, g)] = second_pass(core, g, 1)

    def choose_query(g):
        x_rest(qx, qx_sem, g)
        for p in (0, 1):
            for j in range(4):
                c = j * HD
                qsel[p * 2 + g, c:c + HD, :] = pick(lambda d: qx[d, p, g, :, c:c + HD], p)

    def swap_end():
        for g in (0, 1):
            arrived(out_ref.at[:, columns_of(other, g)], out_sem.at[g])

    def finish_sends():
        for copy in sends:
            copy.wait_send()

    x_send(kst, kx, kx_sem, 0)
    loads[1].wait()
    loads[4].start()
    values = project(1)
    for h in range(2):
        for g in range(2):
            c = (h * 2 + g) * HD
            vst[h, g] = values[:, c:c + HD].T.astype(BF)
    vx[0, core] = vst[core]
    x_send(vst, vx, vx_sem, 0)
    loads[2].wait()
    loads[5].start()
    query_block(0)
    x_relay(kx, kx_sem, 0)
    x_send(kst, kx, kx_sem, 1)
    loads[3].wait()
    query_block(1)
    x_relay(vx, vx_sem, 0)
    x_send(vst, vx, vx_sem, 1)
    flags_arrived()
    loads[4].wait()
    query_block(2)
    begin(chunks[0])
    x_relay(kx, kx_sem, 1)
    loads[5].wait()
    query_block(3)
    qx[0, core] = qst[core]
    begin(chunks[1])
    x_relay(vx, vx_sem, 1)
    x_send(qst, qx, qx_sem, 0)
    x_send(qst, qx, qx_sem, 1)
    near(chunks[0])
    begin(chunks[2])
    near(chunks[1])
    begin(chunks[3])
    far(chunks[0])
    near(chunks[2])
    far(chunks[1])
    near(chunks[3])
    x_relay(qx, qx_sem, 0)
    cross(chunks[0])
    far(chunks[2])
    for j in range(32):
        code_ref[j] = seq_ref[row, j] * 16 + ord_ref[row, j]
    lax.fori_loop(0, 32, look_up, 0)
    cross(chunks[1])
    far(chunks[3])
    x_relay(qx, qx_sem, 1)
    cross(chunks[2])
    choose_query(0)
    last(chunks[0])
    first_pass(other, 0, 0)
    first_pass(core, 0, 1)
    cross(chunks[3])
    last(chunks[1])
    give(0)
    keep(0)
    choose_query(1)
    last(chunks[2])

    def score_side(i, carry):
        first_pass(jnp.where(i == 0, other, core), 1, i)
        return carry

    lax.fori_loop(0, 2, score_side, 0)
    last(chunks[3])
    give(1)
    keep(1)
    swap_end()
    finish_sends()


def local(tokens, qkv_weight, owner_slot, slab_sequence, slab_order):
    hbm = pl.BlockSpec(memory_space=pltpu.HBM)
    dma = pltpu.SemaphoreType.DMA
    pin = functools.partial(pltpu.with_memory_space_constraint, memory_space=pltpu.HBM)
    out = pl.pallas_call(
        kernel,
        out_shape=jax.ShapeDtypeStruct((SLAB, QH * HD), BF),
        in_specs=[pl.BlockSpec(memory_space=pltpu.SMEM)] + [hbm] * 5,
        out_specs=pl.BlockSpec(memory_space=pltpu.VMEM),
        scratch_shapes=[
            pltpu.SMEM((4, 32), jnp.int32),
            pltpu.SMEM((4, 32), jnp.int32),
            pltpu.VMEM((SLAB, D), BF),
            pltpu.VMEM((6, D, 512), BF),
            pltpu.VMEM((288, HD), F32),
            pltpu.VMEM((2, 2, SLAB, HD), BF),
            pltpu.VMEM((2, 2, HD, SLAB), BF),
            pltpu.VMEM((2, 2, SLAB, 512), BF),
            pltpu.VMEM((4, 2, 2, SLAB, HD), BF),
            pltpu.VMEM((4, 2, 2, HD, SLAB), BF),
            pltpu.VMEM((4, 2, 2, SLAB, 512), BF),
            pltpu.VMEM((32, SLAB, HD), BF),
            pltpu.VMEM((32, SLAB, HD), BF),
            pltpu.VMEM((32, HD, SLAB), BF),
            pltpu.VMEM((32, HD, SLAB), BF),
            pltpu.VMEM((4, 2, 8, 128), jnp.int32),
            pltpu.VMEM((4, 512, HD), BF),
            pltpu.VMEM((2, 8, 2, SLAB, 512), F32),
            pltpu.VMEM((2, 1, 512), F32),
            pltpu.VMEM((2, SLAB, 512), BF),
            pltpu.SMEM((32,), jnp.int32),
            pltpu.SMEM((2, 16), jnp.int32),
            dma((10,)),
            dma((131,)),
            dma((4, 2)),
            dma((2, 4, 2)),
            dma((2, 4, 2)),
            dma((2, 4, 2)),
            dma((2, 4, 4, 2)),
            dma((2, 4, 4, 2)),
            dma((2,)),
        ],
        compiler_params=pltpu.CompilerParams(
            collective_id=0, has_side_effects=True, vmem_limit_bytes=46 * 1024 * 1024
        ),
        name="slab_attention",
    )(owner_slot, pin(slab_sequence), pin(slab_order), pin(tokens[0]), qkv_weight, pin(jnp.asarray(rope_tables())))
    return out[None]


def solution(mesh):
    in_specs = (P("dp", "cp", None), P(), P("dp", "cp"), P(), P())
    out_specs = P("dp", "cp", None)
    return jax.shard_map(local, mesh=mesh, in_specs=in_specs, out_specs=out_specs, check_vma=False)
```

```python
import functools
import math

import jax
import jax.numpy as jnp
import numpy as np
from jax import lax
from jax.experimental import pallas as pl
from jax.experimental.pallas import tpu as pltpu
from jax.sharding import PartitionSpec as P

QH = 16
KVH = 4
HD = 128
D = 4096
SLAB = 128
ROPE_BASE = 500000.0
NEG = 1e30
RING = 4
BF = jnp.bfloat16
F32 = jnp.float32
SCALE2 = HD ** (-0.5) * math.log2(math.e)


def rope_tables():
    freq = ROPE_BASE ** (-np.arange(64, dtype=np.float64) * 2.0 / HD)
    freq = np.concatenate([freq, freq])[None, :]
    sign = np.where(np.arange(HD) < 64, -1.0, 1.0)[None, :]
    low = np.arange(SLAB, dtype=np.float64)[:, None] * freq
    high = np.arange(16, dtype=np.float64)[:, None] * SLAB * freq
    table = np.concatenate([np.cos(low), np.sin(low) * sign, np.cos(high), np.sin(high) * sign])
    return table.astype(np.float32)


def kernel(
    own_ref, seq_hbm, ord_hbm, x_hbm, w_hbm, tab_hbm, out_ref,
    seq_ref, ord_ref,
    xv, wv, tab, kst, vst, qst, kx, vx, qx, kbuf0, kbuf1, vbuf0, vbuf1, flag, qsel, sbuf, mbuf, ost, code_ref, pick_ref,
    local_sem, send_sem, flag_sem, kx_sem, vx_sem, qx_sem, kg_sem, vg_sem, out_sem,
):
    row = lax.axis_index("dp")
    cp = lax.axis_index("cp")
    core = lax.rem(cp, 2)
    chip = cp // 2
    y = lax.rem(chip, RING)
    z = chip // RING
    other = 1 - core
    first = y * other + z * core
    second = z * other + y * core

    def cp_of(first_at, second_at, which_core):
        y_at = first_at * other + second_at * core
        z_at = second_at * other + first_at * core
        return (z_at * RING + y_at) * 2 + which_core

    def x_peer(shift, which_core):
        return (lax.rem(row + shift, RING), chip * 2 + which_core)

    def plane_peer(df, ds):
        return (row, cp_of(lax.rem(first + df, RING), lax.rem(second + ds, RING), core))

    def piece_col(df, ds):
        return cp_of(lax.rem(first + df, RING), lax.rem(second + ds, RING), 0)

    sends = []

    def send(src, dst, sem, peer):
        copy = pltpu.make_async_remote_copy(
            src_ref=src, dst_ref=dst, send_sem=send_sem.at[len(sends)], recv_sem=sem,
            device_id=peer, device_id_type=pl.DeviceIdType.MESH,
        )
        copy.start()
        sends.append(copy)

    def arrived(dst, sem):
        pltpu.make_async_remote_copy(
            src_ref=dst, dst_ref=dst, send_sem=send_sem.at[0], recv_sem=sem,
            device_id=(row, cp), device_id_type=pl.DeviceIdType.MESH,
        ).wait_recv()

    columns = [2048, 2560, 0, 512, 1024, 1536]
    loads = [
        pltpu.make_async_copy(w_hbm.at[:, pl.ds(c, 512)], wv.at[i], local_sem.at[i])
        for i, c in enumerate(columns)
    ]
    x_load = pltpu.make_async_copy(x_hbm, xv, local_sem.at[6])
    tab_load = pltpu.make_async_copy(tab_hbm, tab, local_sem.at[7])
    small = [
        pltpu.make_async_copy(src, dst, local_sem.at[8 + i])
        for i, (src, dst) in enumerate(((seq_hbm, seq_ref), (ord_hbm, ord_ref)))
    ]
    for copy in small:
        copy.start()
    tab_load.start()
    x_load.start()
    loads[0].start()

    barrier = pltpu.get_barrier_semaphore()
    peers = [(row, chip * 2 + other)]
    for which in (0, 1):
        peers += [x_peer(shift, which) for shift in (1, 2, 3)]
    for shift in (1, 3):
        peers += [plane_peer(shift, 0), plane_peer(0, shift)]
    for peer in peers:
        pl.semaphore_signal(barrier, inc=1, device_id=peer, device_id_type=pl.DeviceIdType.MESH)

    for copy in small:
        copy.wait()
    target = own_ref[0, 0]
    order = ord_ref[target, cp]
    flag[0, core] = jnp.full((8, 128), target, jnp.int32)
    tab_load.wait()
    cos_low, sin_low = tab[0:128, :], tab[128:256, :]
    cos_high = tab[pl.ds(256 + order, 1), :]
    sin_high = tab[pl.ds(272 + order, 1), :]
    cosine = cos_low * cos_high - sin_low * sin_high
    sine = sin_low * cos_high + cos_low * sin_high

    def rope(head):
        return (head * cosine + pltpu.roll(head, 64, 1) * sine).astype(BF)

    def project(block):
        return jnp.dot(xv[...], wv[block], preferred_element_type=F32)

    x_load.wait()
    loads[1].start()
    loads[0].wait()
    loads[2].start()
    loads[3].start()
    keys = project(0)
    for h in range(2):
        for g in range(2):
            c = (h * 2 + g) * HD
            kst[h, g] = rope(keys[:, c:c + HD])
    kx[0, core] = kst[core]
    pl.semaphore_wait(barrier, len(peers))

    send(flag.at[0, core], flag.at[0, core], flag_sem.at[0, 0], (row, chip * 2 + other))
    for shift in (1, 2, 3):
        back = RING - shift
        for which in (0, 1):
            send(flag.at[0, core], flag.at[back, core], flag_sem.at[back, core], x_peer(shift, which))

    def x_send(stage, xbuf, sem, g, halves=(0, 1)):
        for which in halves:
            send(stage.at[which, g], xbuf.at[3, core, g], sem.at[g, 3, core], x_peer(1, which))
            send(stage.at[which, g], xbuf.at[1, core, g], sem.at[g, 1, core], x_peer(3, which))
        if 0 in halves:
            send(stage.at[other, g], xbuf.at[0, core, g], sem.at[g, 0, 0], (row, chip * 2 + other))

    def x_relay(xbuf, sem, g):
        arrived(xbuf.at[3, 0, g], sem.at[g, 3, 0])
        send(xbuf.at[3, 0, g], xbuf.at[2, 0, g], sem.at[g, 2, 0], x_peer(1, core))
        arrived(xbuf.at[1, 1, g], sem.at[g, 1, 1])
        send(xbuf.at[1, 1, g], xbuf.at[2, 1, g], sem.at[g, 2, 1], x_peer(3, core))

    def x_rest(xbuf, sem, g):
        arrived(xbuf.at[0, other, g], sem.at[g, 0, 0])
        arrived(xbuf.at[3, 1, g], sem.at[g, 3, 1])
        arrived(xbuf.at[1, 0, g], sem.at[g, 1, 0])
        arrived(xbuf.at[2, 0, g], sem.at[g, 2, 0])
        arrived(xbuf.at[2, 1, g], sem.at[g, 2, 1])

    my_col = chip * 2
    kbuf, vbuf = (kbuf0, kbuf1), (vbuf0, vbuf1)

    def query_block(i):
        block = project(2 + i)
        for j in range(4):
            qst[i // 2, i % 2, :, j * HD:(j + 1) * HD] = rope(block[:, j * HD:(j + 1) * HD])

    def look_up(i, carry):
        wanted = seq_ref[row, my_col + i // 16] * 16 + lax.rem(i, 16)
        found = 0
        for j in range(32):
            found = jnp.where(code_ref[j] == wanted, j, found)
        pick_ref[i // 16, lax.rem(i, 16)] = found
        return carry

    def flags_arrived():
        arrived(flag.at[0, other], flag_sem.at[0, 0])
        for d in (1, 2, 3):
            for p in (0, 1):
                arrived(flag.at[d, p], flag_sem.at[d, p])

    def pick(parts, p):
        total = None
        for d in range(RING):
            chosen = flag[d, p, 0:1, :] == row
            part = parts(d)
            wide = jnp.broadcast_to(chosen, part.shape)
            total = jnp.where(wide, part, jnp.zeros_like(part) if total is None else total)
        return total

    chunks = [(kx, kx_sem, kbuf, kg_sem, 0), (vx, vx_sem, vbuf, vg_sem, 0),
              (kx, kx_sem, kbuf, kg_sem, 1), (vx, vx_sem, vbuf, vg_sem, 1)]

    def slot_of(buf, g, df, ds, which):
        col = piece_col(df, ds)
        return buf[g].at[pl.ds(col, 2)] if which is None else buf[g].at[pl.ds(col + which, 1)]

    def hop(chunk, df, ds, step_f, step_s, which=None):
        _, _, buf, gsem, g = chunk
        at = (df - step_f) % RING, (ds - step_s) % RING
        slot = slot_of(buf, g, df, ds, which)
        send(slot, slot, gsem.at[g, at[0], at[1], which or 0], plane_peer(step_f % RING, step_s % RING))

    def landed(chunk, df, ds, which=None):
        _, _, buf, gsem, g = chunk
        arrived(slot_of(buf, g, df, ds, which), gsem.at[g, df, ds, which or 0])

    def begin(chunk):
        xbuf, sem, buf, gsem, g = chunk
        x_rest(xbuf, sem, g)
        for p in (0, 1):
            buf[g][my_col + p] = pick(lambda d: xbuf[d, p, g], p)
        hop(chunk, 0, 0, 1, 0)
        hop(chunk, 0, 0, -1, 0)
        hop(chunk, 0, 0, 0, 1)
        hop(chunk, 0, 0, 0, -1)

    def near(chunk):
        landed(chunk, 3, 0)
        hop(chunk, 3, 0, 1, 0, 0)
        hop(chunk, 3, 0, 0, 1)
        hop(chunk, 3, 0, 0, -1)
        landed(chunk, 1, 0)
        hop(chunk, 1, 0, -1, 0, 1)
        hop(chunk, 1, 0, 0, 1)
        hop(chunk, 1, 0, 0, -1)

    def far(chunk):
        landed(chunk, 2, 0, 0)
        landed(chunk, 2, 0, 1)
        hop(chunk, 2, 0, 0, 1)
        hop(chunk, 2, 0, 0, -1)

    def cross(chunk):
        for df in (0, 3, 1, 2):
            landed(chunk, df, 3)
            hop(chunk, df, 3, 0, 1, 0)
            landed(chunk, df, 1)
            hop(chunk, df, 1, 0, -1, 1)

    def last(chunk):
        for df in range(RING):
            landed(chunk, df, 2, 0)
            landed(chunk, df, 2, 1)

    def slabs_of(t, p, own):
        if t == 0:
            cols = (my_col + p, pick_ref[p, 14])
            later = (0.0, jnp.where(own > 14, 0.0, NEG).astype(F32))
        else:
            cols = (pick_ref[p, 2 * t - 2], pick_ref[p, 2 * t - 1])
            later = tuple(jnp.where(own > o, 0.0, NEG).astype(F32) for o in (2 * t - 2, 2 * t - 1))
        return cols, later

    def scores_of(t, p, g, own, query):
        cols, later = slabs_of(t, p, own)
        key = jnp.concatenate([kbuf[g][cols[0]], kbuf[g][cols[1]]], axis=0)
        scores = lax.dot_general(key, query, (((1,), (1,)), ((), ())), preferred_element_type=F32)
        scores = scores * SCALE2
        halves = [scores[:SLAB], scores[SLAB:]]
        if t == 0:
            key_at = lax.broadcasted_iota(jnp.int32, (SLAB, 4 * SLAB), 0)
            query_at = lax.rem(lax.broadcasted_iota(jnp.int32, (SLAB, 4 * SLAB), 1), SLAB)
            halves[0] = jnp.where(key_at <= query_at, halves[0], -NEG)
        return cols, later, halves

    def first_pass(p, g, at):
        own = ord_ref[row, my_col + p]
        query = qsel[p * 2 + g]
        peak = None
        for t in range(8):
            cols, later, halves = scores_of(t, p, g, own, query)
            for i in (0, 1):
                sbuf[at, t, i] = halves[i]
                top = jnp.max(halves[i].reshape(16, 8, 512), axis=0) - later[i]
                peak = top if peak is None else jnp.maximum(peak, top)
        mbuf[at] = jnp.max(peak, axis=0, keepdims=True)

    def second_pass(p, g, at):
        own = ord_ref[row, my_col + p]
        base = mbuf[at]
        total, product = None, None
        for t in range(8):
            cols, later = slabs_of(t, p, own)
            parts = []
            for i in (0, 1):
                weight = jnp.exp2(sbuf[at, t, i] - (base + later[i]))
                part = jnp.sum(weight.reshape(16, 8, 512), axis=0)
                total = part if total is None else total + part
                parts.append(weight.astype(BF))
            value = jnp.concatenate([vbuf[g][cols[0]], vbuf[g][cols[1]]], axis=1)
            term = jnp.dot(value, jnp.concatenate(parts, axis=0), preferred_element_type=F32)
            product = term if product is None else product + term
        result = product / jnp.sum(total, axis=0, keepdims=True)
        return jnp.concatenate([result[:, j * HD:(j + 1) * HD].T.astype(BF) for j in range(4)], axis=1)

    def columns_of(half, g):
        return pl.ds(pl.multiple_of(half * 1024 + g * 512, 512), 512)

    def give(g):
        ost[g] = second_pass(other, g, 0)
        send(ost.at[g], out_ref.at[:, columns_of(core, g)], out_sem.at[g], (row, chip * 2 + other))

    def keep(g):
        out_ref[:, columns_of(core, g)] = second_pass(core, g, 1)

    def choose_query(g):
        x_rest(qx, qx_sem, g)
        for p in (0, 1):
            for j in range(4):
                c = j * HD
                qsel[p * 2 + g, c:c + HD, :] = pick(lambda d: qx[d, p, g, :, c:c + HD], p)

    def swap_end():
        for g in (0, 1):
            arrived(out_ref.at[:, columns_of(other, g)], out_sem.at[g])

    def finish_sends():
        for copy in sends:
            copy.wait_send()

    x_send(kst, kx, kx_sem, 0)
    loads[1].wait()
    loads[4].start()
    values = project(1)
    for h in range(2):
        for g in range(2):
            c = (h * 2 + g) * HD
            vst[h, g] = values[:, c:c + HD].T.astype(BF)
    vx[0, core] = vst[core]
    x_send(vst, vx, vx_sem, 0)
    loads[2].wait()
    loads[5].start()
    query_block(0)
    x_relay(kx, kx_sem, 0)
    loads[3].wait()
    query_block(1)
    x_relay(vx, vx_sem, 0)
    x_send(kst, kx, kx_sem, 1)
    x_send(vst, vx, vx_sem, 1)
    flags_arrived()
    loads[4].wait()
    query_block(2)
    begin(chunks[0])
    x_relay(kx, kx_sem, 1)
    loads[5].wait()
    query_block(3)
    qx[0, core] = qst[core]
    begin(chunks[1])
    x_relay(vx, vx_sem, 1)
    x_send(qst, qx, qx_sem, 0)
    x_send(qst, qx, qx_sem, 1)
    near(chunks[0])
    begin(chunks[2])
    near(chunks[1])
    begin(chunks[3])
    far(chunks[0])
    near(chunks[2])
    far(chunks[1])
    near(chunks[3])
    x_relay(qx, qx_sem, 0)
    cross(chunks[0])
    far(chunks[2])
    for j in range(32):
        code_ref[j] = seq_ref[row, j] * 16 + ord_ref[row, j]
    lax.fori_loop(0, 32, look_up, 0)
    cross(chunks[1])
    far(chunks[3])
    x_relay(qx, qx_sem, 1)
    cross(chunks[2])
    choose_query(0)
    last(chunks[0])
    first_pass(other, 0, 0)
    first_pass(core, 0, 1)
    cross(chunks[3])
    last(chunks[1])
    give(0)
    keep(0)
    choose_query(1)
    last(chunks[2])

    def score_side(i, carry):
        first_pass(jnp.where(i == 0, other, core), 1, i)
        return carry

    lax.fori_loop(0, 2, score_side, 0)
    last(chunks[3])
    give(1)
    keep(1)
    swap_end()
    finish_sends()


def local(tokens, qkv_weight, owner_slot, slab_sequence, slab_order):
    hbm = pl.BlockSpec(memory_space=pltpu.HBM)
    dma = pltpu.SemaphoreType.DMA
    pin = functools.partial(pltpu.with_memory_space_constraint, memory_space=pltpu.HBM)
    out = pl.pallas_call(
        kernel,
        out_shape=jax.ShapeDtypeStruct((SLAB, QH * HD), BF),
        in_specs=[pl.BlockSpec(memory_space=pltpu.SMEM)] + [hbm] * 5,
        out_specs=pl.BlockSpec(memory_space=pltpu.VMEM),
        scratch_shapes=[
            pltpu.SMEM((4, 32), jnp.int32),
            pltpu.SMEM((4, 32), jnp.int32),
            pltpu.VMEM((SLAB, D), BF),
            pltpu.VMEM((6, D, 512), BF),
            pltpu.VMEM((288, HD), F32),
            pltpu.VMEM((2, 2, SLAB, HD), BF),
            pltpu.VMEM((2, 2, HD, SLAB), BF),
            pltpu.VMEM((2, 2, SLAB, 512), BF),
            pltpu.VMEM((4, 2, 2, SLAB, HD), BF),
            pltpu.VMEM((4, 2, 2, HD, SLAB), BF),
            pltpu.VMEM((4, 2, 2, SLAB, 512), BF),
            pltpu.VMEM((32, SLAB, HD), BF),
            pltpu.VMEM((32, SLAB, HD), BF),
            pltpu.VMEM((32, HD, SLAB), BF),
            pltpu.VMEM((32, HD, SLAB), BF),
            pltpu.VMEM((4, 2, 8, 128), jnp.int32),
            pltpu.VMEM((4, 512, HD), BF),
            pltpu.VMEM((2, 8, 2, SLAB, 512), F32),
            pltpu.VMEM((2, 1, 512), F32),
            pltpu.VMEM((2, SLAB, 512), BF),
            pltpu.SMEM((32,), jnp.int32),
            pltpu.SMEM((2, 16), jnp.int32),
            dma((10,)),
            dma((131,)),
            dma((4, 2)),
            dma((2, 4, 2)),
            dma((2, 4, 2)),
            dma((2, 4, 2)),
            dma((2, 4, 4, 2)),
            dma((2, 4, 4, 2)),
            dma((2,)),
        ],
        compiler_params=pltpu.CompilerParams(
            collective_id=0, has_side_effects=True, vmem_limit_bytes=46 * 1024 * 1024
        ),
        name="slab_attention",
    )(owner_slot, pin(slab_sequence), pin(slab_order), pin(tokens[0]), qkv_weight, pin(jnp.asarray(rope_tables())))
    return out[None]


def solution(mesh):
    in_specs = (P("dp", "cp", None), P(), P("dp", "cp"), P(), P())
    out_specs = P("dp", "cp", None)
    return jax.shard_map(local, mesh=mesh, in_specs=in_specs, out_specs=out_specs, check_vma=False)
```

```python
import functools
import math

import jax
import jax.numpy as jnp
import numpy as np
from jax import lax
from jax.experimental import pallas as pl
from jax.experimental.pallas import tpu as pltpu
from jax.sharding import PartitionSpec as P

QH = 16
KVH = 4
HD = 128
D = 4096
SLAB = 128
ROPE_BASE = 500000.0
NEG = 1e30
RING = 4
BF = jnp.bfloat16
F32 = jnp.float32
SCALE2 = HD ** (-0.5) * math.log2(math.e)


def rope_tables():
    freq = ROPE_BASE ** (-np.arange(64, dtype=np.float64) * 2.0 / HD)
    freq = np.concatenate([freq, freq])[None, :]
    sign = np.where(np.arange(HD) < 64, -1.0, 1.0)[None, :]
    low = np.arange(SLAB, dtype=np.float64)[:, None] * freq
    high = np.arange(16, dtype=np.float64)[:, None] * SLAB * freq
    table = np.concatenate([np.cos(low), np.sin(low) * sign, np.cos(high), np.sin(high) * sign])
    return table.astype(np.float32)


def kernel(
    own_ref, seq_hbm, ord_hbm, x_hbm, w_hbm, tab_hbm, out_ref,
    seq_ref, ord_ref,
    xv, wv, tab, kst, vst, qst, kx, vx, qx, kbuf0, kbuf1, vbuf0, vbuf1, flag, qsel, sbuf, mbuf, ost, code_ref, pick_ref,
    local_sem, send_sem, flag_sem, kx_sem, vx_sem, qx_sem, kg_sem, vg_sem, out_sem,
):
    row = lax.axis_index("dp")
    cp = lax.axis_index("cp")
    core = lax.rem(cp, 2)
    chip = cp // 2
    y = lax.rem(chip, RING)
    z = chip // RING
    other = 1 - core
    first = y * other + z * core
    second = z * other + y * core

    def cp_of(first_at, second_at, which_core):
        y_at = first_at * other + second_at * core
        z_at = second_at * other + first_at * core
        return (z_at * RING + y_at) * 2 + which_core

    def x_peer(shift, which_core):
        return (lax.rem(row + shift, RING), chip * 2 + which_core)

    def plane_peer(df, ds):
        return (row, cp_of(lax.rem(first + df, RING), lax.rem(second + ds, RING), core))

    def piece_col(df, ds):
        return cp_of(lax.rem(first + df, RING), lax.rem(second + ds, RING), 0)

    sends = []

    def send(src, dst, sem, peer):
        copy = pltpu.make_async_remote_copy(
            src_ref=src, dst_ref=dst, send_sem=send_sem.at[len(sends)], recv_sem=sem,
            device_id=peer, device_id_type=pl.DeviceIdType.MESH,
        )
        copy.start()
        sends.append(copy)

    def arrived(dst, sem):
        pltpu.make_async_remote_copy(
            src_ref=dst, dst_ref=dst, send_sem=send_sem.at[0], recv_sem=sem,
            device_id=(row, cp), device_id_type=pl.DeviceIdType.MESH,
        ).wait_recv()

    columns = [2048, 2560, 0, 512, 1024, 1536]
    loads = [
        pltpu.make_async_copy(w_hbm.at[:, pl.ds(c, 512)], wv.at[i], local_sem.at[i])
        for i, c in enumerate(columns)
    ]
    x_load = pltpu.make_async_copy(x_hbm, xv, local_sem.at[6])
    tab_load = pltpu.make_async_copy(tab_hbm, tab, local_sem.at[7])
    small = [
        pltpu.make_async_copy(src, dst, local_sem.at[8 + i])
        for i, (src, dst) in enumerate(((seq_hbm, seq_ref), (ord_hbm, ord_ref)))
    ]
    for copy in small:
        copy.start()
    x_load.start()
    loads[0].start()
    tab_load.start()
    loads[1].start()

    barrier = pltpu.get_barrier_semaphore()
    peers = [(row, chip * 2 + other)]
    for which in (0, 1):
        peers += [x_peer(shift, which) for shift in (1, 2, 3)]
    for shift in (1, 3):
        peers += [plane_peer(shift, 0), plane_peer(0, shift)]
    for peer in peers:
        pl.semaphore_signal(barrier, inc=1, device_id=peer, device_id_type=pl.DeviceIdType.MESH)

    for copy in small:
        copy.wait()
    target = own_ref[0, 0]
    order = ord_ref[target, cp]
    flag[0, core] = jnp.full((8, 128), target, jnp.int32)
    tab_load.wait()
    cos_low, sin_low = tab[0:128, :], tab[128:256, :]
    cos_high = tab[pl.ds(256 + order, 1), :]
    sin_high = tab[pl.ds(272 + order, 1), :]
    cosine = cos_low * cos_high - sin_low * sin_high
    sine = sin_low * cos_high + cos_low * sin_high

    def rope(head):
        return (head * cosine + pltpu.roll(head, 64, 1) * sine).astype(BF)

    def project(block):
        return jnp.dot(xv[...], wv[block], preferred_element_type=F32)

    x_load.wait()
    loads[0].wait()
    loads[2].start()
    loads[3].start()
    keys = project(0)
    for h in range(2):
        for g in range(2):
            c = (h * 2 + g) * HD
            kst[h, g] = rope(keys[:, c:c + HD])
    kx[0, core] = kst[core]
    pl.semaphore_wait(barrier, len(peers))

    send(flag.at[0, core], flag.at[0, core], flag_sem.at[0, 0], (row, chip * 2 + other))
    for shift in (1, 2, 3):
        back = RING - shift
        for which in (0, 1):
            send(flag.at[0, core], flag.at[back, core], flag_sem.at[back, core], x_peer(shift, which))

    def x_send(stage, xbuf, sem, g, halves=(0, 1)):
        for which in halves:
            send(stage.at[which, g], xbuf.at[3, core, g], sem.at[g, 3, core], x_peer(1, which))
            send(stage.at[which, g], xbuf.at[1, core, g], sem.at[g, 1, core], x_peer(3, which))
        if 0 in halves:
            send(stage.at[other, g], xbuf.at[0, core, g], sem.at[g, 0, 0], (row, chip * 2 + other))

    def x_relay(xbuf, sem, g):
        arrived(xbuf.at[3, 0, g], sem.at[g, 3, 0])
        send(xbuf.at[3, 0, g], xbuf.at[2, 0, g], sem.at[g, 2, 0], x_peer(1, core))
        arrived(xbuf.at[1, 1, g], sem.at[g, 1, 1])
        send(xbuf.at[1, 1, g], xbuf.at[2, 1, g], sem.at[g, 2, 1], x_peer(3, core))

    def x_rest(xbuf, sem, g):
        arrived(xbuf.at[0, other, g], sem.at[g, 0, 0])
        arrived(xbuf.at[3, 1, g], sem.at[g, 3, 1])
        arrived(xbuf.at[1, 0, g], sem.at[g, 1, 0])
        arrived(xbuf.at[2, 0, g], sem.at[g, 2, 0])
        arrived(xbuf.at[2, 1, g], sem.at[g, 2, 1])

    my_col = chip * 2
    kbuf, vbuf = (kbuf0, kbuf1), (vbuf0, vbuf1)

    def query_block(i):
        block = project(2 + i)
        for j in range(4):
            qst[i // 2, i % 2, :, j * HD:(j + 1) * HD] = rope(block[:, j * HD:(j + 1) * HD])

    def look_up(i, carry):
        wanted = seq_ref[row, my_col + i // 16] * 16 + lax.rem(i, 16)
        found = 0
        for j in range(32):
            found = jnp.where(code_ref[j] == wanted, j, found)
        pick_ref[i // 16, lax.rem(i, 16)] = found
        return carry

    def flags_arrived():
        arrived(flag.at[0, other], flag_sem.at[0, 0])
        for d in (1, 2, 3):
            for p in (0, 1):
                arrived(flag.at[d, p], flag_sem.at[d, p])

    def pick(parts, p):
        total = None
        for d in range(RING):
            chosen = flag[d, p, 0:1, :] == row
            part = parts(d)
            wide = jnp.broadcast_to(chosen, part.shape)
            total = jnp.where(wide, part, jnp.zeros_like(part) if total is None else total)
        return total

    chunks = [(kx, kx_sem, kbuf, kg_sem, 0), (vx, vx_sem, vbuf, vg_sem, 0),
              (kx, kx_sem, kbuf, kg_sem, 1), (vx, vx_sem, vbuf, vg_sem, 1)]

    def slot_of(buf, g, df, ds, which):
        col = piece_col(df, ds)
        return buf[g].at[pl.ds(col, 2)] if which is None else buf[g].at[pl.ds(col + which, 1)]

    def hop(chunk, df, ds, step_f, step_s, which=None):
        _, _, buf, gsem, g = chunk
        at = (df - step_f) % RING, (ds - step_s) % RING
        slot = slot_of(buf, g, df, ds, which)
        send(slot, slot, gsem.at[g, at[0], at[1], which or 0], plane_peer(step_f % RING, step_s % RING))

    def landed(chunk, df, ds, which=None):
        _, _, buf, gsem, g = chunk
        arrived(slot_of(buf, g, df, ds, which), gsem.at[g, df, ds, which or 0])

    def begin(chunk):
        xbuf, sem, buf, gsem, g = chunk
        x_rest(xbuf, sem, g)
        for p in (0, 1):
            buf[g][my_col + p] = pick(lambda d: xbuf[d, p, g], p)
        hop(chunk, 0, 0, 1, 0)
        hop(chunk, 0, 0, -1, 0)
        hop(chunk, 0, 0, 0, 1)
        hop(chunk, 0, 0, 0, -1)

    def near(chunk):
        landed(chunk, 3, 0)
        hop(chunk, 3, 0, 1, 0, 0)
        hop(chunk, 3, 0, 0, 1)
        hop(chunk, 3, 0, 0, -1)
        landed(chunk, 1, 0)
        hop(chunk, 1, 0, -1, 0, 1)
        hop(chunk, 1, 0, 0, 1)
        hop(chunk, 1, 0, 0, -1)

    def far(chunk):
        landed(chunk, 2, 0, 0)
        landed(chunk, 2, 0, 1)
        hop(chunk, 2, 0, 0, 1)
        hop(chunk, 2, 0, 0, -1)

    def cross(chunk):
        for df in (0, 3, 1, 2):
            landed(chunk, df, 3)
            hop(chunk, df, 3, 0, 1, 0)
            landed(chunk, df, 1)
            hop(chunk, df, 1, 0, -1, 1)

    def last(chunk):
        for df in range(RING):
            landed(chunk, df, 2, 0)
            landed(chunk, df, 2, 1)

    def slabs_of(t, p, own):
        if t == 0:
            cols = (my_col + p, pick_ref[p, 14])
            later = (0.0, jnp.where(own > 14, 0.0, NEG).astype(F32))
        else:
            cols = (pick_ref[p, 2 * t - 2], pick_ref[p, 2 * t - 1])
            later = tuple(jnp.where(own > o, 0.0, NEG).astype(F32) for o in (2 * t - 2, 2 * t - 1))
        return cols, later

    def scores_of(t, p, g, own, query):
        cols, later = slabs_of(t, p, own)
        key = jnp.concatenate([kbuf[g][cols[0]], kbuf[g][cols[1]]], axis=0)
        scores = lax.dot_general(key, query, (((1,), (1,)), ((), ())), preferred_element_type=F32)
        scores = scores * SCALE2
        halves = [scores[:SLAB], scores[SLAB:]]
        if t == 0:
            key_at = lax.broadcasted_iota(jnp.int32, (SLAB, 4 * SLAB), 0)
            query_at = lax.rem(lax.broadcasted_iota(jnp.int32, (SLAB, 4 * SLAB), 1), SLAB)
            halves[0] = jnp.where(key_at <= query_at, halves[0], -NEG)
        return cols, later, halves

    def first_pass(p, g, at):
        own = ord_ref[row, my_col + p]
        query = qsel[p * 2 + g]
        peak = None
        for t in range(8):
            cols, later, halves = scores_of(t, p, g, own, query)
            for i in (0, 1):
                sbuf[at, t, i] = halves[i]
                top = jnp.max(halves[i].reshape(16, 8, 512), axis=0) - later[i]
                peak = top if peak is None else jnp.maximum(peak, top)
        mbuf[at] = jnp.max(peak, axis=0, keepdims=True)

    def second_pass(p, g, at):
        own = ord_ref[row, my_col + p]
        base = mbuf[at]
        total, product = None, None
        for t in range(8):
            cols, later = slabs_of(t, p, own)
            parts = []
            for i in (0, 1):
                weight = jnp.exp2(sbuf[at, t, i] - (base + later[i]))
                part = jnp.sum(weight.reshape(16, 8, 512), axis=0)
                total = part if total is None else total + part
                parts.append(weight.astype(BF))
            value = jnp.concatenate([vbuf[g][cols[0]], vbuf[g][cols[1]]], axis=1)
            term = jnp.dot(value, jnp.concatenate(parts, axis=0), preferred_element_type=F32)
            product = term if product is None else product + term
        result = product / jnp.sum(total, axis=0, keepdims=True)
        return jnp.concatenate([result[:, j * HD:(j + 1) * HD].T.astype(BF) for j in range(4)], axis=1)

    def columns_of(half, g):
        return pl.ds(pl.multiple_of(half * 1024 + g * 512, 512), 512)

    def give(g):
        ost[g] = second_pass(other, g, 0)
        send(ost.at[g], out_ref.at[:, columns_of(core, g)], out_sem.at[g], (row, chip * 2 + other))

    def keep(g):
        out_ref[:, columns_of(core, g)] = second_pass(core, g, 1)

    def choose_query(g):
        x_rest(qx, qx_sem, g)
        for p in (0, 1):
            for j in range(4):
                c = j * HD
                qsel[p * 2 + g, c:c + HD, :] = pick(lambda d: qx[d, p, g, :, c:c + HD], p)

    def swap_end():
        for g in (0, 1):
            arrived(out_ref.at[:, columns_of(other, g)], out_sem.at[g])

    def finish_sends():
        for copy in sends:
            copy.wait_send()

    x_send(kst, kx, kx_sem, 0)
    loads[1].wait()
    loads[4].start()
    values = project(1)
    for h in range(2):
        for g in range(2):
            c = (h * 2 + g) * HD
            vst[h, g] = values[:, c:c + HD].T.astype(BF)
    vx[0, core] = vst[core]
    x_send(vst, vx, vx_sem, 0)
    loads[2].wait()
    loads[5].start()
    query_block(0)
    x_relay(kx, kx_sem, 0)
    x_send(kst, kx, kx_sem, 1)
    loads[3].wait()
    query_block(1)
    x_relay(vx, vx_sem, 0)
    x_send(vst, vx, vx_sem, 1)
    flags_arrived()
    loads[4].wait()
    query_block(2)
    begin(chunks[0])
    x_relay(kx, kx_sem, 1)
    loads[5].wait()
    query_block(3)
    qx[0, core] = qst[core]
    begin(chunks[1])
    x_relay(vx, vx_sem, 1)
    x_send(qst, qx, qx_sem, 0)
    x_send(qst, qx, qx_sem, 1)
    near(chunks[0])
    begin(chunks[2])
    near(chunks[1])
    begin(chunks[3])
    far(chunks[0])
    near(chunks[2])
    far(chunks[1])
    near(chunks[3])
    x_relay(qx, qx_sem, 0)
    cross(chunks[0])
    far(chunks[2])
    for j in range(32):
        code_ref[j] = seq_ref[row, j] * 16 + ord_ref[row, j]
    lax.fori_loop(0, 32, look_up, 0)
    cross(chunks[1])
    far(chunks[3])
    x_relay(qx, qx_sem, 1)
    cross(chunks[2])
    choose_query(0)
    last(chunks[0])
    first_pass(other, 0, 0)
    first_pass(core, 0, 1)
    cross(chunks[3])
    last(chunks[1])
    give(0)
    keep(0)
    choose_query(1)
    last(chunks[2])

    def score_side(i, carry):
        first_pass(jnp.where(i == 0, other, core), 1, i)
        return carry

    lax.fori_loop(0, 2, score_side, 0)
    last(chunks[3])
    give(1)
    keep(1)
    swap_end()
    finish_sends()


def local(tokens, qkv_weight, owner_slot, slab_sequence, slab_order):
    hbm = pl.BlockSpec(memory_space=pltpu.HBM)
    dma = pltpu.SemaphoreType.DMA
    pin = functools.partial(pltpu.with_memory_space_constraint, memory_space=pltpu.HBM)
    out = pl.pallas_call(
        kernel,
        out_shape=jax.ShapeDtypeStruct((SLAB, QH * HD), BF),
        in_specs=[pl.BlockSpec(memory_space=pltpu.SMEM)] + [hbm] * 5,
        out_specs=pl.BlockSpec(memory_space=pltpu.VMEM),
        scratch_shapes=[
            pltpu.SMEM((4, 32), jnp.int32),
            pltpu.SMEM((4, 32), jnp.int32),
            pltpu.VMEM((SLAB, D), BF),
            pltpu.VMEM((6, D, 512), BF),
            pltpu.VMEM((288, HD), F32),
            pltpu.VMEM((2, 2, SLAB, HD), BF),
            pltpu.VMEM((2, 2, HD, SLAB), BF),
            pltpu.VMEM((2, 2, SLAB, 512), BF),
            pltpu.VMEM((4, 2, 2, SLAB, HD), BF),
            pltpu.VMEM((4, 2, 2, HD, SLAB), BF),
            pltpu.VMEM((4, 2, 2, SLAB, 512), BF),
            pltpu.VMEM((32, SLAB, HD), BF),
            pltpu.VMEM((32, SLAB, HD), BF),
            pltpu.VMEM((32, HD, SLAB), BF),
            pltpu.VMEM((32, HD, SLAB), BF),
            pltpu.VMEM((4, 2, 8, 128), jnp.int32),
            pltpu.VMEM((4, 512, HD), BF),
            pltpu.VMEM((2, 8, 2, SLAB, 512), F32),
            pltpu.VMEM((2, 1, 512), F32),
            pltpu.VMEM((2, SLAB, 512), BF),
            pltpu.SMEM((32,), jnp.int32),
            pltpu.SMEM((2, 16), jnp.int32),
            dma((10,)),
            dma((131,)),
            dma((4, 2)),
            dma((2, 4, 2)),
            dma((2, 4, 2)),
            dma((2, 4, 2)),
            dma((2, 4, 4, 2)),
            dma((2, 4, 4, 2)),
            dma((2,)),
        ],
        compiler_params=pltpu.CompilerParams(
            collective_id=0, has_side_effects=True, vmem_limit_bytes=46 * 1024 * 1024
        ),
        name="slab_attention",
    )(owner_slot, pin(slab_sequence), pin(slab_order), pin(tokens[0]), qkv_weight, pin(jnp.asarray(rope_tables())))
    return out[None]


def solution(mesh):
    in_specs = (P("dp", "cp", None), P(), P("dp", "cp"), P(), P())
    out_specs = P("dp", "cp", None)
    return jax.shard_map(local, mesh=mesh, in_specs=in_specs, out_specs=out_specs, check_vma=False)
```
